32 devices in a mesh: row: 8 (over y, x, core), col: 4 (over z).
Axes of the slice: x: 2, y: 2, z: 4, core: 2. Of those that a mesh axis runs over, the one named last changes fastest.
Arguments:
- state: float32 [2048, 4, 1024], P('row', 'col'), may hold values from -6 to 6
- coupling: bfloat16 [2048, 4, 1024], P('row', 'col'), may hold values from -2 to 2, as said below
- coupling_t: bfloat16 [2, 2048, 4, 1024], P(None, 'row', 'col'), may hold values from -2 to 2, as said below
- factor: float32 [4, 4, 256, 256], P(None, 'col', 'row'), may hold values from -0.3 to 1.3
- cofactor: float32 [4, 4, 256, 256], P(None, 'col', 'row'), may hold values from -0.3 to 1.3
- rates: float32 [4, 4, 256], P(None, 'col'), may hold values from 0.5 to 2
Outputs:
- updated_state: float32 [2048, 4, 1024], P('row', 'col')
The draws below stay inside these ranges and needn't reach their ends.
Inputs may be any that keep to these rules, and one draw needn't show every extreme that they name: coupling and coupling_t hold the same matrix A; its blocks A(i, k) are zero unless k > i. coupling_t holds the transposed blocks of the A in coupling.
All inputs are finite; a program needn't handle non-finite values.
Results may differ from the reference program's by a relative error of at most 0.0003.
Values may be sent and summed in bfloat16 or wider, within the bound.
A program may use at most 64 MiB of HBM per device.

```python
import math
import jax
import jax.numpy as jnp
from jax import lax

BS = 256
STEPS = 2
NBH = 8
NB = 16
CB = 4
N_COL = 4


def coupling_blocks(seed_key, block_rows, block_cols):
    base_key = jax.random.fold_in(seed_key, 404)
    flat_rows = block_rows.reshape(-1).astype(jnp.int32)
    flat_cols = block_cols.reshape(-1).astype(jnp.int32)
    limit = 4.0 / math.sqrt(BS)

    def one_block(row_id, col_id):
        sub_key = jax.random.fold_in(base_key, row_id * NB + col_id)
        values = jax.random.normal(sub_key, (BS, BS), jnp.float32) / math.sqrt(BS)
        values = jnp.clip(values, -limit, limit)
        return jnp.where(col_id > row_id, values, 0.0)
    drawn = jax.vmap(one_block)(flat_rows, flat_cols)
    return drawn.reshape(block_rows.shape + (BS, BS))


def draw_coupling(key, part):
    col_count = NB // CB
    row_ids = jnp.arange(NBH, dtype=jnp.int32)[:, None, None]
    stored = (jnp.arange(CB, dtype=jnp.int32)[:, None] * col_count + jnp.arange(col_count, dtype=jnp.int32)[None, :])[None]
    block_rows = jnp.broadcast_to(row_ids, (NBH, CB, col_count))
    block_cols = jnp.broadcast_to(NB - 1 - stored, (NBH, CB, col_count))
    drawn = coupling_blocks(key, block_rows, block_cols)
    drawn = jnp.transpose(drawn, (0, 3, 2, 1, 4))
    return drawn.reshape(NBH * BS, col_count, CB * BS).astype(jnp.bfloat16)


def draw_coupling_t(key, part):
    col_count = NB // CB
    rotated = (jnp.arange(NBH, dtype=jnp.int32) + NBH // 2) % NBH
    stored_rows = jnp.arange(2, dtype=jnp.int32)[:, None] * NBH + rotated[None, :]
    stored_cols = jnp.arange(CB, dtype=jnp.int32)[:, None] * col_count + jnp.arange(col_count, dtype=jnp.int32)[None, :]
    block_rows = jnp.broadcast_to(stored_cols[None, None], (2, NBH, CB, col_count))
    block_cols = jnp.broadcast_to((NB - 1 - stored_rows)[:, :, None, None], (2, NBH, CB, col_count))
    drawn = coupling_blocks(key, block_rows, block_cols)
    drawn = jnp.swapaxes(drawn, -1, -2)
    drawn = jnp.transpose(drawn, (0, 1, 4, 3, 2, 5))
    return drawn.reshape(2, NBH * BS, col_count, CB * BS).astype(jnp.bfloat16)


def operator_draw(seed_key):
    col_count = NB // CB
    perturb = jax.random.normal(seed_key, (CB, col_count, BS, BS), jnp.float32)
    perturb = jnp.clip(0.3 * perturb / math.sqrt(BS), -0.3, 0.3)
    return jnp.eye(BS, dtype=jnp.float32) + perturb


def draw_factor(key, part):
    return operator_draw(jax.random.fold_in(key, 17))


def draw_cofactor(key, part):
    return operator_draw(jax.random.fold_in(key, 29))


def block_scale(own_key, dims, shards, least, largest):
    gain = 1.0
    for axis_at, blocks in shards:
        steps = jax.random.uniform(jax.random.fold_in(jax.random.fold_in(own_key, 6), axis_at), (blocks,), jnp.float32, least / len(shards), largest / len(shards))
        gain = gain * jnp.repeat(jnp.exp(steps), dims[axis_at] // blocks).reshape((-1,) + (1,) * (len(dims) - 1 - axis_at))
    return gain


def centred(stream_key, dims, scale, bound, pieces=(), held_as=jnp.bfloat16):
    entries = jax.random.normal(stream_key, dims, jnp.float32) * scale
    if len(pieces) > 0:
        entries = block_scale(stream_key, dims, pieces, -0.22, 0.18) * entries
    return jnp.clip(entries, min=-bound, max=bound).astype(held_as)


def setup_inputs(seed: int = 0) -> dict:
    key_list = jax.random.split(jax.random.key(seed), 7)
    state = centred(key_list[0], (NBH * BS, N_COL, CB * BS), 1.0, 6.0, ((0, 8), (1, 4)), jnp.float32)
    coupling = draw_coupling(jax.random.fold_in(key_list[6], 71), 0)
    coupling_t = draw_coupling_t(jax.random.fold_in(key_list[6], 71), 0)
    factor = draw_factor(jax.random.fold_in(key_list[6], 71), 0)
    cofactor = draw_cofactor(jax.random.fold_in(key_list[6], 71), 0)
    rates = jnp.clip(jnp.exp(math.log(2.0) - 1.3862944 * jax.random.uniform(key_list[5], (CB, N_COL, BS), jnp.float32) ** block_scale(key_list[5], (CB, N_COL, BS), ((1, 4),), -0.2, 0.2)), 0.5, 2.0)
    return {"state": state, "coupling": coupling, "coupling_t": coupling_t, "factor": factor, "cofactor": cofactor, "rates": rates}


HIGHEST_PRECISION = lax.Precision.HIGHEST


def to_blocks(flattened, row_total):
    col_count = flattened.shape[1]
    shaped = flattened.reshape(row_total, BS, col_count, CB, BS)
    shaped = jnp.transpose(shaped, (0, 3, 2, 1, 4))
    return shaped.reshape(row_total, CB * col_count, BS, BS)


def from_blocks(blocks):
    row_total = blocks.shape[0]
    col_count = blocks.shape[1] // CB
    shaped = blocks.reshape(row_total, CB, col_count, BS, BS)
    shaped = jnp.transpose(shaped, (0, 3, 2, 1, 4))
    return shaped.reshape(row_total * BS, col_count, CB * BS)


def solve_block(residual, left_p, left_q, left_e, right_p, right_q, right_e):
    middle = jnp.dot(left_q, residual, precision=HIGHEST_PRECISION, preferred_element_type=jnp.float32)
    middle = jnp.dot(middle, right_q.T, precision=HIGHEST_PRECISION, preferred_element_type=jnp.float32)
    middle = middle / (left_e[:, None] + right_e[None, :])
    product = jnp.dot(left_p, middle, precision=HIGHEST_PRECISION, preferred_element_type=jnp.float32)
    return -jnp.dot(product, right_p.T, precision=HIGHEST_PRECISION, preferred_element_type=jnp.float32)


def reference(state, coupling, coupling_t, factor, cofactor, rates):
    col_count = state.shape[1]
    half_rows = NBH // 2
    blocks = to_blocks(state, NBH)
    upper_blocks = to_blocks(coupling, NBH)
    lower_blocks = to_blocks(coupling_t.reshape(NB * BS, col_count, CB * BS), NB)
    all_p = factor.reshape(NB, BS, BS)
    all_q = cofactor.reshape(NB, BS, BS)
    all_e = rates.reshape(NB, BS)
    row_ids = jnp.arange(NBH, dtype=jnp.int32)
    col_ids = jnp.arange(NB, dtype=jnp.int32)
    for wave_step in range(STEPS):
        antidiag = NB - 1 - wave_step
        partner = (antidiag - row_ids).astype(jnp.int32)
        usable = row_ids <= partner
        residual = blocks[row_ids, partner]
        solution = jax.vmap(solve_block)(residual, all_p[:NBH], all_q[:NBH], all_e[:NBH], all_p[partner], all_q[partner], all_e[partner])
        solution = jnp.where(usable[:, None, None], solution, 0.0)
        blocks = blocks.at[row_ids, partner].set(jnp.where(usable[:, None, None], solution, residual))
        mirror = (antidiag - col_ids).astype(jnp.int32)
        use_row = mirror <= col_ids
        sources = jnp.clip(jnp.where(use_row, mirror, col_ids), 0, NBH - 1).astype(jnp.int32)
        chosen = solution[sources]
        partner_blocks = jnp.where(use_row[:, None, None], chosen, jnp.swapaxes(chosen, 1, 2))
        upper_pick = jnp.clip(wave_step + col_ids, 0, NB - 1).astype(jnp.int32)

        def update_row(row_args, wave_step=wave_step, antidiag=antidiag, partner_blocks=partner_blocks, upper_pick=upper_pick):
            row_id, row_blocks, row_solution = row_args
            needed = wave_step + row_id
            stored = ((needed % NBH + half_rows) % NBH + NBH * (needed // NBH)).astype(jnp.int32)
            coupled = upper_blocks[row_id][upper_pick].astype(jnp.float32)
            transposed = lower_blocks[stored].astype(jnp.float32)
            left_terms = jnp.einsum("mab,mbc->mac", coupled, partner_blocks, precision=HIGHEST_PRECISION)
            right_terms = jnp.einsum("ab,mbc->mac", row_solution, transposed, precision=HIGHEST_PRECISION)
            targets = (row_id <= col_ids) & (row_id + col_ids < antidiag)
            return row_blocks - jnp.where(targets[:, None, None], left_terms + right_terms, 0.0)

        blocks = lax.map(update_row, (row_ids, blocks, solution))
    return from_blocks(blocks)
```

```python
import functools

import jax
import jax.numpy as jnp
from jax import lax
from jax.experimental import pallas as pl
from jax.experimental.pallas import tpu as pltpu
from jax.sharding import PartitionSpec as P

STEPS = 2
MESH = pl.DeviceIdType.MESH
F32 = jnp.float32
NN = (((1,), (0,)), ((), ()))
NT = (((1,), (1,)), ((), ()))


def halves(x):
    hi = x.astype(jnp.bfloat16)
    return hi, (x - hi.astype(F32)).astype(jnp.bfloat16)


def mm(a, b, dims):
    return lax.dot_general(a, b, dims, preferred_element_type=F32)


def dot3(a, b, dims):
    ah, al = halves(a)
    bh, bl = halves(b)
    return mm(ah, bh, dims) + (mm(ah, bl, dims) + mm(al, bh, dims))


def kernel(R, C, U, BS, SR, state, upper, lower, factor, cofactor, rates, out,
           ops, ebuf, xz, atb, an, ops_sem, e_sem, xz_sem, at_sem, an_sem, send_sem):
    H = R // 2
    r = lax.axis_index("row")
    c = lax.axis_index("col")
    d = [2 * R - 1 - s for s in range(STEPS)]

    def owner(row, s):
        return (d[s] - row) % C

    o = [owner(r, s) for s in range(STEPS)]
    sends = []

    def send(cond, src, dst, sem, dev):
        k = len(sends)
        copy = pltpu.make_async_remote_copy(
            src_ref=src, dst_ref=dst, send_sem=send_sem.at[k], recv_sem=sem,
            device_id=dev, device_id_type=MESH)
        sends.append((cond, copy))

        @pl.when(cond)
        def _():
            copy.start()

    def send_or_local(cond, src, dst, sem, dev):
        mine = (dev[0] == r) & (dev[1] == c)
        send(cond & jnp.logical_not(mine), src, dst, sem, dev)

        @pl.when(cond & mine)
        def _():
            pltpu.make_async_copy(src, dst, sem).start()

    def arrive(ref, sem):
        pltpu.make_async_copy(ref, ref, sem).wait()

    def slot(u):
        if isinstance(u, int):
            return pl.ds(u * BS, BS)
        return pl.ds(pl.multiple_of(u * BS, BS), BS)

    def target(row, m, s):
        return (row <= m) & (row + m < d[s])

    rows = pl.ds(pl.multiple_of(r * SR, SR), SR)
    for src, base in ((cofactor, 0), (factor, 2)):
        for s in range(STEPS):
            for u in range(U):
                m = c + C * u
                if u >= U // 2 - s:
                    to = d[s] - m
                    send_or_local((to >= 0) & (to < R), src.at[u], ops.at[base + 1, rows],
                                  ops_sem.at[base + 1], (to, c))
                if u < U // 2:
                    send_or_local(m < R, src.at[u], ops.at[base, rows],
                                  ops_sem.at[base], (m, owner(m, s)))
    for s in range(STEPS):
        send_or_local(c == r % C, rates, ebuf, e_sem.at[0], (r, o[s]))

    def send_lower(s):
        to = (r + R - s - H) % R
        for u in reversed(range(U)):
            m = c + C * u
            send(target(to, m, s) & (to + s < R), lower.at[:, slot(u)], atb.at[s, u],
                 at_sem.at[s, u], (to, c))

    def send_upper():
        for u in range(U):
            m = c + C * u - 1
            to = (c + C - 1) % C
            to_u = jnp.maximum(jnp.where(c >= 1, u, u - 1), 0)
            send((m >= 0) & target(r, m, 1), upper.at[:, slot(u)], an.at[to_u],
                 an_sem.at[to_u], (r, to))

    send_lower(0)
    send_upper()
    out[...] = state[...]

    def spread(s):
        own_col = r % C == c
        k = jnp.where(own_col, r // C, (d[s] - r) // C)
        for back in range(1, R):
            to = jnp.maximum(r - back, 0)
            send((r >= back) & (own_col | (c == o[s])), xz.at[s, U], xz.at[s, k],
                 xz_sem.at[s, k], (to, c))

    def share_row(s):
        for hop in range(1, C):
            to = (c + C - hop) % C
            send(c == o[s], xz.at[s, U], xz.at[s, U], xz_sem.at[s, U], (r, to))

    def solve(s):
        q = (d[s] - r) // C
        arrive(ebuf, e_sem.at[0])
        left_e = jnp.transpose(jnp.broadcast_to(ebuf[pl.ds(r // C, 1), :], (BS, BS)))
        rate = left_e + rates[pl.ds(q, 1), :]
        arrive(ops.at[0], ops_sem.at[0])
        mid = dot3(ops[0], out[:, slot(q)], NN)
        arrive(ops.at[1], ops_sem.at[1])
        mid = dot3(mid, ops[1], NT) / rate
        arrive(ops.at[2], ops_sem.at[2])
        mid = dot3(ops[2], mid, NN)
        arrive(ops.at[3], ops_sem.at[3])
        x = -dot3(mid, ops[3], NT)
        xz[s, U] = x
        out[:, slot(q)] = x

    def z_index(u, s):
        m = c + C * u
        j = jnp.where(d[s] - m <= m, d[s] - m, m)
        k = jnp.where(j == r, U, jnp.where(j % C == c, j // C, u))
        return j, k

    def await_z(u, s):
        j, k = z_index(u, s)
        landed = r < j
        if u >= U // 2:
            landed = landed & (j % C != c)

        @pl.when(landed)
        def _():
            arrive(xz.at[s, u], xz_sem.at[s, u])

    def update(u, s):
        m = c + C * u
        j, k = z_index(u, s)
        arrive(atb.at[s, u], at_sem.at[s, u])
        if s > 0:
            arrive(an.at[u], an_sem.at[u])
            a = an[u]
        else:
            a = upper[:, slot(u)]
        xh, xl = halves(xz[s, U])
        at = atb[s, u]
        out[:, slot(u)] -= mm(xh, at, NN) + mm(xl, at, NN)
        zh, zl = halves(xz[s, k])
        straight = d[s] - m <= m

        @pl.when(straight)
        def _():
            out[:, slot(u)] -= mm(a, zh, NN) + mm(a, zl, NN)

        @pl.when(jnp.logical_not(straight))
        def _():
            out[:, slot(u)] -= mm(a, zh, NT) + mm(a, zl, NT)

    def step_update(u, s):
        await_z(u, s)

        @pl.when(target(r, c + C * u, s))
        def _():
            update(u, s)

    @pl.when(c == o[0])
    def _():
        solve(0)

    @pl.when(c != o[0])
    def _():
        arrive(xz.at[0, U], xz_sem.at[0, U])

    share_row(0)
    spread(0)
    send_lower(1)

    q1 = (d[1] - r) // C
    first = c == o[1]
    for u in range(U // 2 - 1, U):
        @pl.when(first & (q1 == u))
        def _(u=u):
            step_update(u, 0)

    @pl.when(first)
    def _():
        solve(1)

    share_row(1)

    def rest():
        for u in range(U):
            skip = first & (q1 == u)

            @pl.when(jnp.logical_not(skip))
            def _(u=u):
                step_update(u, 0)

    @pl.when(jnp.logical_not(first))
    def _():
        rest()
        arrive(xz.at[1, U], xz_sem.at[1, U])

    spread(1)

    @pl.when(first)
    def _():
        rest()

    for u in range(U):
        step_update(u, 1)

    for cond, copy in sends:
        @pl.when(cond)
        def _(copy=copy):
            copy.wait_send()


def on_device(state, coupling, coupling_t, factor, cofactor, rates):
    R = lax.axis_size("row")
    C = lax.axis_size("col")
    U = 2 * R // C
    BS = state.shape[0]
    SR = factor.shape[2]
    flat = U * BS
    vmem = pl.BlockSpec(memory_space=pltpu.VMEM)
    n_sends = 2 * STEPS * (2 * U) + STEPS + (STEPS + 1) * U + STEPS * (R - 1 + C - 1)
    dma = pltpu.SemaphoreType.DMA
    out = pl.pallas_call(
        functools.partial(kernel, R, C, U, BS, SR),
        out_shape=jax.ShapeDtypeStruct((BS, flat), F32),
        in_specs=[vmem] * 6,
        out_specs=vmem,
        scratch_shapes=[
            pltpu.VMEM((4, BS, BS), F32),
            pltpu.VMEM((U, BS), F32),
            pltpu.VMEM((STEPS, U + 1, BS, BS), F32),
            pltpu.VMEM((STEPS, U, BS, BS), jnp.bfloat16),
            pltpu.VMEM((U, BS, BS), jnp.bfloat16),
            dma((4,)),
            dma((1,)),
            dma((STEPS, U + 1)),
            dma((STEPS, U)),
            dma((U,)),
            dma((n_sends,)),
        ],
        compiler_params=pltpu.CompilerParams(
            has_side_effects=True, vmem_limit_bytes=48 * 1024 * 1024),
    )(
        state.reshape(BS, flat),
        coupling.reshape(BS, flat),
        coupling_t[0].reshape(BS, flat),
        factor.reshape(U, SR, BS),
        cofactor.reshape(U, SR, BS),
        rates.reshape(U, BS),
    )
    return out.reshape(BS, 1, flat)


def solution(mesh):
    return jax.shard_map(
        on_device,
        mesh=mesh,
        in_specs=(
            P("row", "col", None),
            P("row", "col", None),
            P(None, "row", "col", None),
            P(None, "col", "row", None),
            P(None, "col", "row", None),
            P(None, "col", None),
        ),
        out_specs=P("row", "col", None),
        check_vma=False,
    )
```

```python
import functools

import jax
import jax.numpy as jnp
from jax import lax
from jax.experimental import pallas as pl
from jax.experimental.pallas import tpu as pltpu
from jax.sharding import PartitionSpec as P

STEPS = 2
MESH = pl.DeviceIdType.MESH
F32 = jnp.float32
NN = (((1,), (0,)), ((), ()))
NT = (((1,), (1,)), ((), ()))


def halves(x):
    hi = x.astype(jnp.bfloat16)
    return hi, (x - hi.astype(F32)).astype(jnp.bfloat16)


def mm(a, b, dims):
    return lax.dot_general(a, b, dims, preferred_element_type=F32)


def dot3(a, b, dims):
    ah, al = halves(a)
    bh, bl = halves(b)
    return mm(ah, bh, dims) + (mm(ah, bl, dims) + mm(al, bh, dims))


def kernel(R, C, U, BS, SR, state, upper, lower, factor, cofactor, rates, out,
           ops, ebuf, xz, atb, an, ops_sem, e_sem, xz_sem, at_sem, an_sem, send_sem):
    H = R // 2
    r = lax.axis_index("row")
    c = lax.axis_index("col")
    d = [2 * R - 1 - s for s in range(STEPS)]

    def owner(row, s):
        return (d[s] - row) % C

    o = [owner(r, s) for s in range(STEPS)]
    sends = []

    def send(cond, src, dst, sem, dev):
        k = len(sends)
        copy = pltpu.make_async_remote_copy(
            src_ref=src, dst_ref=dst, send_sem=send_sem.at[k], recv_sem=sem,
            device_id=dev, device_id_type=MESH)
        sends.append((cond, copy))

        @pl.when(cond)
        def _():
            copy.start()

    def send_or_local(cond, src, dst, sem, dev):
        mine = (dev[0] == r) & (dev[1] == c)
        send(cond & jnp.logical_not(mine), src, dst, sem, dev)

        @pl.when(cond & mine)
        def _():
            pltpu.make_async_copy(src, dst, sem).start()

    def arrive(ref, sem):
        pltpu.make_async_copy(ref, ref, sem).wait()

    def slot(u):
        if isinstance(u, int):
            return pl.ds(u * BS, BS)
        return pl.ds(pl.multiple_of(u * BS, BS), BS)

    def target(row, m, s):
        return (row <= m) & (row + m < d[s])

    def wants_row(col, s):
        hit = col == r % C
        for u in range(U):
            hit = hit | target(r, col + C * u, s)
        return hit

    rows = pl.ds(pl.multiple_of(r * SR, SR), SR)

    def send_operators(s):
        for src, base in ((cofactor, 0), (factor, 2)):
            for u in range(U):
                m = c + C * u
                if u >= U // 2 - s:
                    to = d[s] - m
                    send_or_local((to >= 0) & (to < R), src.at[u], ops.at[base + 1, rows],
                                  ops_sem.at[base + 1], (to, c))
                if u < U // 2:
                    send_or_local(m < R, src.at[u], ops.at[base, rows],
                                  ops_sem.at[base], (m, owner(m, s)))

    def from_upper(u):
        return (u + 1) * C <= H

    def send_lower(s, slots):
        to = (r + R - s - H) % R
        for u in slots:
            if not from_upper(u):
                m = c + C * u
                send(target(to, m, s) & (to + s < R), lower.at[:, slot(u)], atb.at[s, u],
                     at_sem.at[s, u], (to, c))

    def send_plain(s):
        m = r
        to_u = jnp.minimum(m // C, U - 1)
        for u in range(H // C + 1):
            i = c + C * u - s
            reach = (i >= 0) & (m < (H // C) * C) & target(i, m, s)
            send_or_local(reach, upper.at[:, slot(u)], atb.at[s, to_u],
                          at_sem.at[s, to_u], (i, m % C))

    def send_upper():
        for u in range(U):
            m = c + C * u - 1
            to = (c + C - 1) % C
            to_u = jnp.maximum(jnp.where(c >= 1, u, u - 1), 0)
            send((m >= 0) & target(r, m, 1), upper.at[:, slot(u)], an.at[to_u],
                 an_sem.at[to_u], (r, to))

    for s in range(STEPS):
        send_or_local(c == r % C, rates, ebuf, e_sem.at[0], (r, o[s]))
    send_operators(0)
    send_operators(1)
    send_lower(0, range(U - 1, U // 2 - 1, -1))
    send_plain(0)
    out[...] = state[...]

    def spread(s, who=True):
        own_col = r % C == c
        k = jnp.where(own_col, r // C, (d[s] - r) // C)
        has = (own_col | (c == o[s])) & who

        def give(cond, to):
            send(cond & has, xz.at[s, U], xz.at[s, k], xz_sem.at[s, k], (to, c))

        give(r % 2 == 1, jnp.maximum(r - 1, 0))
        for back in range(1, R // 2):
            pair = r // 2 - back
            give(pair >= 0, jnp.maximum(2 * pair + 1 - r % 2, 0))

    def share_row(s):
        for hop in range(1, C):
            to = (c + C - hop) % C
            send((c == o[s]) & wants_row(to, s), xz.at[s, U], xz.at[s, U], xz_sem.at[s, U], (r, to))

    def await_row(s):
        @pl.when(wants_row(c, s))
        def _():
            arrive(xz.at[s, U], xz_sem.at[s, U])

    def solve(s):
        q = (d[s] - r) // C
        arrive(ebuf, e_sem.at[0])
        left_e = jnp.transpose(jnp.broadcast_to(ebuf[pl.ds(r // C, 1), :], (BS, BS)))
        rate = left_e + rates[pl.ds(q, 1), :]
        arrive(ops.at[0], ops_sem.at[0])
        mid = dot3(ops[0], out[:, slot(q)], NN)
        arrive(ops.at[1], ops_sem.at[1])
        mid = dot3(mid, ops[1], NT) / rate
        arrive(ops.at[2], ops_sem.at[2])
        mid = dot3(ops[2], mid, NN)
        arrive(ops.at[3], ops_sem.at[3])
        x = -dot3(mid, ops[3], NT)
        xz[s, U] = x
        out[:, slot(q)] = x

    def z_index(u, s):
        m = c + C * u
        j = jnp.where(d[s] - m <= m, d[s] - m, m)
        k = jnp.where(j == r, U, jnp.where(j % C == c, j // C, u))
        return j, k

    def collect(u, s, extra=True):
        j, k = z_index(u, s)
        landed = r < j
        if u >= U // 2:
            landed = landed & (j % C != c)
        landed = landed & extra

        @pl.when(landed)
        def _():
            arrive(xz.at[s, u], xz_sem.at[s, u])

        send(landed & (r // 2 < j // 2) & (r % 2 != j % 2), xz.at[s, u], xz.at[s, u],
             xz_sem.at[s, u], (r + 1 - 2 * (r % 2), c))

    def right(u, s):
        arrive(atb.at[s, u], at_sem.at[s, u])
        xh, xl = halves(xz[s, U])
        at = atb[s, u]
        dims = NT if from_upper(u) else NN
        out[:, slot(u)] -= mm(xh, at, dims) + mm(xl, at, dims)

    def left(u, s):
        m = c + C * u
        j, k = z_index(u, s)
        if s > 0:
            arrive(an.at[u], an_sem.at[u])
            a = an[u]
        else:
            a = upper[:, slot(u)]
        zh, zl = halves(xz[s, k])

        def apply(dims):
            out[:, slot(u)] -= mm(a, zh, dims) + mm(a, zl, dims)

        low, high = C * u, C * u + C - 1
        if 2 * low >= d[s]:
            apply(NN)
        elif 2 * high < d[s]:
            apply(NT)
        else:
            straight = d[s] - m <= m
            pl.when(straight)(lambda: apply(NN))
            pl.when(jnp.logical_not(straight))(lambda: apply(NT))

    def on_targets(s, fns, but=None):
        for u in range(U):
            live = target(r, c + C * u, s)
            if but is not None:
                live = live & jnp.logical_not(but(u))

            @pl.when(live)
            def _(u=u):
                for fn in fns:
                    fn(u, s)

    @pl.when(c == o[0])
    def _():
        solve(0)

    @pl.when(c != o[0])
    def _():
        await_row(0)

    share_row(0)
    spread(0)
    send_lower(0, range(U // 2 - 1, -1, -1))
    send_upper()
    send_lower(1, range(U - 1, -1, -1))
    send_plain(1)

    q1 = (d[1] - r) // C
    first = c == o[1]

    def picked(u):
        return first & (q1 == u)

    for u in range(U // 2 - 1, U):
        collect(u, 0, picked(u))

        @pl.when(picked(u))
        def _(u=u):
            right(u, 0)
            left(u, 0)

    @pl.when(first)
    def _():
        solve(1)

    share_row(1)

    def rest():
        on_targets(0, (right, left), picked)

    spread(1, first)
    for u in range(U):
        collect(u, 0, jnp.logical_not(picked(u)))
    rest()

    @pl.when(jnp.logical_not(first))
    def _():
        await_row(1)

    spread(1, jnp.logical_not(first))
    on_targets(1, (right,))
    for u in range(U):
        collect(u, 1)
    on_targets(1, (left,))

    for cond, copy in sends:
        @pl.when(cond)
        def _(copy=copy):
            copy.wait_send()


def on_device(state, coupling, coupling_t, factor, cofactor, rates):
    R = lax.axis_size("row")
    C = lax.axis_size("col")
    U = 2 * R // C
    BS = state.shape[0]
    SR = factor.shape[2]
    flat = U * BS
    vmem = pl.BlockSpec(memory_space=pltpu.VMEM)
    n_sends = 2 * STEPS * (2 * U) + (STEPS + 8) * (2 * U) + STEPS * (2 * R + C)
    dma = pltpu.SemaphoreType.DMA
    out = pl.pallas_call(
        functools.partial(kernel, R, C, U, BS, SR),
        out_shape=jax.ShapeDtypeStruct((BS, flat), F32),
        in_specs=[vmem] * 6,
        out_specs=vmem,
        scratch_shapes=[
            pltpu.VMEM((4, BS, BS), F32),
            pltpu.VMEM((U, BS), F32),
            pltpu.VMEM((STEPS, U + 1, BS, BS), F32),
            pltpu.VMEM((STEPS, U, BS, BS), jnp.bfloat16),
            pltpu.VMEM((U, BS, BS), jnp.bfloat16),
            dma((4,)),
            dma((1,)),
            dma((STEPS, U + 1)),
            dma((STEPS, U)),
            dma((U,)),
            dma((n_sends,)),
        ],
        compiler_params=pltpu.CompilerParams(
            has_side_effects=True, vmem_limit_bytes=48 * 1024 * 1024),
    )(
        state.reshape(BS, flat),
        coupling.reshape(BS, flat),
        coupling_t[0].reshape(BS, flat),
        factor.reshape(U, SR, BS),
        cofactor.reshape(U, SR, BS),
        rates.reshape(U, BS),
    )
    return out.reshape(BS, 1, flat)


def solution(mesh):
    return jax.shard_map(
        on_device,
        mesh=mesh,
        in_specs=(
            P("row", "col", None),
            P("row", "col", None),
            P(None, "row", "col", None),
            P(None, "col", "row", None),
            P(None, "col", "row", None),
            P(None, "col", None),
        ),
        out_specs=P("row", "col", None),
        check_vma=False,
    )
```

```python
import functools

import jax
import jax.numpy as jnp
from jax import lax
from jax.experimental import pallas as pl
from jax.experimental.pallas import tpu as pltpu
from jax.sharding import PartitionSpec as P

STEPS = 2
MESH = pl.DeviceIdType.MESH
F32 = jnp.float32
NN = (((1,), (0,)), ((), ()))
NT = (((1,), (1,)), ((), ()))


def halves(x):
    hi = x.astype(jnp.bfloat16)
    return hi, (x - hi.astype(F32)).astype(jnp.bfloat16)


def mm(a, b, dims):
    return lax.dot_general(a, b, dims, preferred_element_type=F32)


def dot3(a, b, dims):
    ah, al = halves(a)
    bh, bl = halves(b)
    return mm(ah, bh, dims) + (mm(ah, bl, dims) + mm(al, bh, dims))


def kernel(R, C, U, BS, SR, state, upper, lower, factor, cofactor, rates, out,
           ops, ebuf, xz, atb, an, ops_sem, e_sem, xz_sem, at_sem, an_sem, send_sem):
    H = R // 2
    r = lax.axis_index("row")
    c = lax.axis_index("col")
    d = [2 * R - 1 - s for s in range(STEPS)]

    def owner(row, s):
        return (d[s] - row) % C

    o = [owner(r, s) for s in range(STEPS)]
    sends = []

    def send(cond, src, dst, sem, dev):
        k = len(sends)
        copy = pltpu.make_async_remote_copy(
            src_ref=src, dst_ref=dst, send_sem=send_sem.at[k], recv_sem=sem,
            device_id=dev, device_id_type=MESH)
        sends.append((cond, copy))

        @pl.when(cond)
        def _():
            copy.start()

    def send_or_local(cond, src, dst, sem, dev):
        mine = (dev[0] == r) & (dev[1] == c)
        send(cond & jnp.logical_not(mine), src, dst, sem, dev)

        @pl.when(cond & mine)
        def _():
            pltpu.make_async_copy(src, dst, sem).start()

    def arrive(ref, sem):
        pltpu.make_async_copy(ref, ref, sem).wait()

    def slot(u):
        if isinstance(u, int):
            return pl.ds(u * BS, BS)
        return pl.ds(pl.multiple_of(u * BS, BS), BS)

    def target(row, m, s):
        return (row <= m) & (row + m < d[s])

    rows = pl.ds(pl.multiple_of(r * SR, SR), SR)

    def send_operators(s):
        for src, base in ((cofactor, 0), (factor, 2)):
            for u in range(U):
                m = c + C * u
                if u >= U // 2 - s:
                    to = d[s] - m
                    send_or_local((to >= 0) & (to < R), src.at[u], ops.at[base + 1, rows],
                                  ops_sem.at[base + 1], (to, c))
                if u < U // 2:
                    send_or_local(m < R, src.at[u], ops.at[base, rows],
                                  ops_sem.at[base], (m, owner(m, s)))

    def from_upper(u):
        return (u + 1) * C <= H

    def send_lower(s, slots):
        to = (r + R - s - H) % R
        for u in slots:
            if not from_upper(u):
                m = c + C * u
                send(target(to, m, s) & (to + s < R), lower.at[:, slot(u)], atb.at[s, u],
                     at_sem.at[s, u], (to, c))

    def send_plain(s):
        m = r
        to_u = jnp.minimum(m // C, U - 1)
        for u in range(H // C + 1):
            i = c + C * u - s
            reach = (i >= 0) & (m < (H // C) * C) & target(i, m, s)
            send_or_local(reach, upper.at[:, slot(u)], atb.at[s, to_u],
                          at_sem.at[s, to_u], (i, m % C))

    def send_upper():
        for u in range(U):
            m = c + C * u - 1
            to = (c + C - 1) % C
            to_u = jnp.maximum(jnp.where(c >= 1, u, u - 1), 0)
            send((m >= 0) & target(r, m, 1), upper.at[:, slot(u)], an.at[to_u],
                 an_sem.at[to_u], (r, to))

    for s in range(STEPS):
        send_or_local(c == r % C, rates, ebuf, e_sem.at[0], (r, o[s]))
    send_operators(0)
    send_operators(1)
    send_upper()
    send_lower(0, range(U - 1, U // 2 - 1, -1))
    send_plain(0)
    out[...] = state[...]

    def spread(s, who=True):
        own_col = r % C == c
        k = jnp.where(own_col, r // C, (d[s] - r) // C)
        has = (own_col | (c == o[s])) & who

        def give(cond, to):
            send(cond & has, xz.at[s, U], xz.at[s, k], xz_sem.at[s, k], (to, c))

        give(r % 2 == 1, jnp.maximum(r - 1, 0))
        for back in range(1, R // 2):
            pair = r // 2 - back
            give(pair >= 0, jnp.maximum(2 * pair + 1 - r % 2, 0))

    def half(h):
        return pl.ds(h * (BS // 2), BS // 2)

    def pass_row(s, h, who=True):
        block = xz.at[s, U, half(h)]
        sem = xz_sem.at[s, U + h]
        far = o[s] == 0
        up = (c >= o[s]) & (c < C - 1)
        if s == 0:
            send((c == o[s]) & far & who, block, block, sem, (r, C - 1))
            up = up & jnp.logical_not(far & (c == C - 2))
        send((c <= o[s]) & (c >= 1) & who, block, block, sem, (r, jnp.maximum(c - 1, 0)))
        send(up & who, block, block, sem, (r, jnp.minimum(c + 1, C - 1)))

    def take_row(s):
        other = c != o[s]
        for h in range(2):
            @pl.when(other)
            def _(h=h):
                arrive(xz.at[s, U, half(h)], xz_sem.at[s, U + h])

            pass_row(s, h, other)

    def give_row(s):
        for h in range(2):
            pass_row(s, h, c == o[s])

    def solve(s):
        q = (d[s] - r) // C
        arrive(ebuf, e_sem.at[0])
        left_e = jnp.transpose(jnp.broadcast_to(ebuf[pl.ds(r // C, 1), :], (BS, BS)))
        rate = left_e + rates[pl.ds(q, 1), :]
        arrive(ops.at[0], ops_sem.at[0])
        mid = dot3(ops[0], out[:, slot(q)], NN)
        arrive(ops.at[1], ops_sem.at[1])
        mid = dot3(mid, ops[1], NT) / rate
        arrive(ops.at[2], ops_sem.at[2])
        mid = dot3(ops[2], mid, NN)
        arrive(ops.at[3], ops_sem.at[3])
        x = -dot3(mid, ops[3], NT)
        xz[s, U] = x
        out[:, slot(q)] = x

    def z_index(u, s):
        m = c + C * u
        j = jnp.where(d[s] - m <= m, d[s] - m, m)
        k = jnp.where(j == r, U, jnp.where(j % C == c, j // C, u))
        return j, k

    def collect(u, s, extra=True):
        j, k = z_index(u, s)
        landed = r < j
        if u >= U // 2:
            landed = landed & (j % C != c)
        landed = landed & extra

        @pl.when(landed)
        def _():
            arrive(xz.at[s, u], xz_sem.at[s, u])

        send(landed & (r // 2 < j // 2) & (r % 2 != j % 2), xz.at[s, u], xz.at[s, u],
             xz_sem.at[s, u], (r + 1 - 2 * (r % 2), c))

    def right(u, s):
        arrive(atb.at[s, u], at_sem.at[s, u])
        xh, xl = halves(xz[s, U])
        at = atb[s, u]
        dims = NT if from_upper(u) else NN
        out[:, slot(u)] -= mm(xh, at, dims) + mm(xl, at, dims)

    def left(u, s):
        m = c + C * u
        j, k = z_index(u, s)
        if s > 0:
            arrive(an.at[u], an_sem.at[u])
            a = an[u]
        else:
            a = upper[:, slot(u)]
        zh, zl = halves(xz[s, k])

        def apply(dims):
            out[:, slot(u)] -= mm(a, zh, dims) + mm(a, zl, dims)

        low, high = C * u, C * u + C - 1
        if 2 * low >= d[s]:
            apply(NN)
        elif 2 * high < d[s]:
            apply(NT)
        else:
            straight = d[s] - m <= m
            pl.when(straight)(lambda: apply(NN))
            pl.when(jnp.logical_not(straight))(lambda: apply(NT))

    def on_targets(s, fns, but=None):
        for u in range(U):
            live = target(r, c + C * u, s)
            if but is not None:
                live = live & jnp.logical_not(but(u))

            @pl.when(live)
            def _(u=u):
                for fn in fns:
                    fn(u, s)

    @pl.when(c == o[0])
    def _():
        solve(0)

    give_row(0)
    take_row(0)
    spread(0)
    send_lower(0, range(U // 2 - 1, -1, -1))
    send_lower(1, range(U - 1, -1, -1))
    send_plain(1)

    q1 = (d[1] - r) // C
    first = c == o[1]

    def picked(u):
        return first & (q1 == u)

    for u in range(U // 2 - 1, U):
        collect(u, 0, picked(u))

        @pl.when(picked(u))
        def _(u=u):
            right(u, 0)
            left(u, 0)

    @pl.when(first)
    def _():
        solve(1)

    give_row(1)

    def rest():
        on_targets(0, (right, left), picked)

    spread(1, first)
    for u in range(U):
        collect(u, 0, jnp.logical_not(picked(u)))
    rest()

    take_row(1)
    spread(1, jnp.logical_not(first))
    on_targets(1, (right,))
    for u in range(U):
        collect(u, 1)
    on_targets(1, (left,))

    for cond, copy in sends:
        @pl.when(cond)
        def _(copy=copy):
            copy.wait_send()


def on_device(state, coupling, coupling_t, factor, cofactor, rates):
    R = lax.axis_size("row")
    C = lax.axis_size("col")
    U = 2 * R // C
    BS = state.shape[0]
    SR = factor.shape[2]
    flat = U * BS
    vmem = pl.BlockSpec(memory_space=pltpu.VMEM)
    n_sends = 2 * STEPS * (2 * U) + (STEPS + 8) * (2 * U) + STEPS * (2 * R + 16)
    dma = pltpu.SemaphoreType.DMA
    out = pl.pallas_call(
        functools.partial(kernel, R, C, U, BS, SR),
        out_shape=jax.ShapeDtypeStruct((BS, flat), F32),
        in_specs=[vmem] * 6,
        out_specs=vmem,
        scratch_shapes=[
            pltpu.VMEM((4, BS, BS), F32),
            pltpu.VMEM((U, BS), F32),
            pltpu.VMEM((STEPS, U + 1, BS, BS), F32),
            pltpu.VMEM((STEPS, U, BS, BS), jnp.bfloat16),
            pltpu.VMEM((U, BS, BS), jnp.bfloat16),
            dma((4,)),
            dma((1,)),
            dma((STEPS, U + 2)),
            dma((STEPS, U)),
            dma((U,)),
            dma((n_sends,)),
        ],
        compiler_params=pltpu.CompilerParams(
            has_side_effects=True, vmem_limit_bytes=48 * 1024 * 1024),
    )(
        state.reshape(BS, flat),
        coupling.reshape(BS, flat),
        coupling_t[0].reshape(BS, flat),
        factor.reshape(U, SR, BS),
        cofactor.reshape(U, SR, BS),
        rates.reshape(U, BS),
    )
    return out.reshape(BS, 1, flat)


def solution(mesh):
    return jax.shard_map(
        on_device,
        mesh=mesh,
        in_specs=(
            P("row", "col", None),
            P("row", "col", None),
            P(None, "row", "col", None),
            P(None, "col", "row", None),
            P(None, "col", "row", None),
            P(None, "col", None),
        ),
        out_specs=P("row", "col", None),
        check_vma=False,
    )
```

```python
import functools

import jax
import jax.numpy as jnp
from jax import lax
from jax.experimental import pallas as pl
from jax.experimental.pallas import tpu as pltpu
from jax.sharding import PartitionSpec as P

STEPS = 2
CHUNKS = 4
MESH = pl.DeviceIdType.MESH
F32 = jnp.float32
NN = (((1,), (0,)), ((), ()))
NT = (((1,), (1,)), ((), ()))


def halves(x):
    hi = x.astype(jnp.bfloat16)
    return hi, (x - hi.astype(F32)).astype(jnp.bfloat16)


def mm(a, b, dims):
    return lax.dot_general(a, b, dims, preferred_element_type=F32)


def dot3(a, b, dims):
    ah, al = halves(a)
    bh, bl = halves(b)
    return mm(ah, bh, dims) + (mm(ah, bl, dims) + mm(al, bh, dims))


def kernel(R, C, U, BS, SR, state, upper, lower, factor, cofactor, rates, out,
           ops, ebuf, xz, atb, an, ops_sem, e_sem, xz_sem, at_sem, an_sem, send_sem):
    H = R // 2
    r = lax.axis_index("row")
    c = lax.axis_index("col")
    d = [2 * R - 1 - s for s in range(STEPS)]

    def owner(row, s):
        return (d[s] - row) % C

    o = [owner(r, s) for s in range(STEPS)]
    sends = []
    me = r * C + c

    barrier = pltpu.get_barrier_semaphore()

    @pl.loop(1, R * C)
    def _(k):
        peer = (me + k) % (R * C)
        pl.semaphore_signal(barrier, inc=1, device_id=(peer // C, peer % C), device_id_type=MESH)

    pl.semaphore_wait(barrier, R * C - 1)

    def send(cond, src, dst, sem, dev):
        k = len(sends)
        copy = pltpu.make_async_remote_copy(
            src_ref=src, dst_ref=dst, send_sem=send_sem.at[k], recv_sem=sem,
            device_id=dev, device_id_type=MESH)
        sends.append((cond, copy))

        @pl.when(cond)
        def _():
            copy.start()

    def send_or_local(cond, src, dst, sem, dev):
        mine = (dev[0] == r) & (dev[1] == c)
        send(cond & jnp.logical_not(mine), src, dst, sem, dev)

        @pl.when(cond & mine)
        def _():
            pltpu.make_async_copy(src, dst, sem).start()

    def arrive(ref, sem):
        pltpu.make_async_copy(ref, ref, sem).wait()

    def slot(u):
        if isinstance(u, int):
            return pl.ds(u * BS, BS)
        return pl.ds(pl.multiple_of(u * BS, BS), BS)

    def target(row, m, s):
        return (row <= m) & (row + m < d[s])

    rows = pl.ds(pl.multiple_of(r * SR, SR), SR)

    def send_operators(s):
        for src, base in ((cofactor, 0), (factor, 2)):
            for u in range(U):
                m = c + C * u
                if u >= U // 2 - s:
                    to = d[s] - m
                    send_or_local((to >= 0) & (to < R), src.at[u], ops.at[base + 1, rows],
                                  ops_sem.at[base + 1], (to, c))
                if u < U // 2:
                    send_or_local(m < R, src.at[u], ops.at[base, rows],
                                  ops_sem.at[base], (m, owner(m, s)))

    def from_upper(u):
        return (u + 1) * C <= H

    def send_lower(s, slots):
        to = (r + R - s - H) % R
        for u in slots:
            if not from_upper(u):
                m = c + C * u
                send(target(to, m, s) & (to + s < R), lower.at[:, slot(u)], atb.at[s, u],
                     at_sem.at[s, u], (to, c))

    def send_plain(s):
        m = r
        to_u = jnp.minimum(m // C, U - 1)
        for u in range(H // C + 1):
            i = c + C * u - s
            reach = (i >= 0) & (m < (H // C) * C) & target(i, m, s)
            send_or_local(reach, upper.at[:, slot(u)], atb.at[s, to_u],
                          at_sem.at[s, to_u], (i, m % C))

    def send_upper():
        for u in range(U):
            m = c + C * u - 1
            to = (c + C - 1) % C
            to_u = jnp.maximum(jnp.where(c >= 1, u, u - 1), 0)
            send((m >= 0) & target(r, m, 1), upper.at[:, slot(u)], an.at[to_u],
                 an_sem.at[to_u], (r, to))

    for s in range(STEPS):
        send_or_local(c == r % C, rates, ebuf, e_sem.at[0], (r, o[s]))
    send_operators(0)
    send_operators(1)
    send_upper()
    send_lower(0, range(U - 1, U // 2 - 1, -1))
    send_plain(0)
    out[...] = state[...]

    def spread(s, h, who):
        own_col = r % C == c
        k = jnp.where(own_col, r // C, (d[s] - r) // C)
        has = (own_col | (c == o[s])) & who

        def give(cond, to):
            send(cond & has, xz.at[s, U, part(h)], xz.at[s, k, part(h)], xz_sem.at[s, k, h], (to, c))

        give(r % 2 == 1, jnp.maximum(r - 1, 0))
        for back in range(1, R // 2):
            pair = r // 2 - back
            give(pair >= 0, jnp.maximum(2 * pair + 1 - r % 2, 0))

    def part(h):
        return pl.ds(h * (BS // CHUNKS), BS // CHUNKS)

    def pass_row(s, h, who=True):
        block = xz.at[s, U, part(h)]
        sem = xz_sem.at[s, U, h]
        far = o[s] == 0
        up = (c >= o[s]) & (c < C - 1)
        if s == 0:
            send((c == o[s]) & far & who, block, block, sem, (r, C - 1))
            up = up & jnp.logical_not(far & (c == C - 2))
        send((c <= o[s]) & (c >= 1) & who, block, block, sem, (r, jnp.maximum(c - 1, 0)))
        send(up & who, block, block, sem, (r, jnp.minimum(c + 1, C - 1)))

    def take_row(s):
        other = c != o[s]
        for h in range(CHUNKS):
            @pl.when(other)
            def _(h=h):
                arrive(xz.at[s, U, part(h)], xz_sem.at[s, U, h])

            pass_row(s, h, other)
            spread(s, h, other)

    def give_row(s):
        for h in range(CHUNKS):
            pass_row(s, h, c == o[s])
            spread(s, h, c == o[s])

    def solve(s):
        q = (d[s] - r) // C
        arrive(ebuf, e_sem.at[0])
        left_e = jnp.transpose(jnp.broadcast_to(ebuf[pl.ds(r // C, 1), :], (BS, BS)))
        rate = left_e + rates[pl.ds(q, 1), :]
        arrive(ops.at[0], ops_sem.at[0])
        mid = dot3(ops[0], out[:, slot(q)], NN)
        arrive(ops.at[1], ops_sem.at[1])
        mid = dot3(mid, ops[1], NT) / rate
        arrive(ops.at[2], ops_sem.at[2])
        mid = dot3(ops[2], mid, NN)
        arrive(ops.at[3], ops_sem.at[3])
        x = -dot3(mid, ops[3], NT)
        xz[s, U] = x
        out[:, slot(q)] = x

    def z_index(u, s):
        m = c + C * u
        j = jnp.where(d[s] - m <= m, d[s] - m, m)
        k = jnp.where(j == r, U, jnp.where(j % C == c, j // C, u))
        return j, k

    def collect(u, s, extra=True):
        j, k = z_index(u, s)
        landed = r < j
        if u >= U // 2:
            landed = landed & (j % C != c)
        landed = landed & extra

        for h in range(CHUNKS):
            block = xz.at[s, u, part(h)]

            @pl.when(landed)
            def _(block=block, h=h):
                arrive(block, xz_sem.at[s, u, h])

            send(landed & (r // 2 < j // 2) & (r % 2 != j % 2), block, block,
                 xz_sem.at[s, u, h], (r + 1 - 2 * (r % 2), c))

    def right(u, s):
        arrive(atb.at[s, u], at_sem.at[s, u])
        xh, xl = halves(xz[s, U])
        at = atb[s, u]
        dims = NT if from_upper(u) else NN
        out[:, slot(u)] -= mm(xh, at, dims) + mm(xl, at, dims)

    def left(u, s):
        m = c + C * u
        j, k = z_index(u, s)
        if s > 0:
            arrive(an.at[u], an_sem.at[u])
            a = an[u]
        else:
            a = upper[:, slot(u)]
        zh, zl = halves(xz[s, k])

        def apply(dims):
            out[:, slot(u)] -= mm(a, zh, dims) + mm(a, zl, dims)

        low, high = C * u, C * u + C - 1
        if 2 * low >= d[s]:
            apply(NN)
        elif 2 * high < d[s]:
            apply(NT)
        else:
            straight = d[s] - m <= m
            pl.when(straight)(lambda: apply(NN))
            pl.when(jnp.logical_not(straight))(lambda: apply(NT))

    def on_targets(s, fns, but=None):
        for u in range(U):
            live = target(r, c + C * u, s)
            if but is not None:
                live = live & jnp.logical_not(but(u))

            @pl.when(live)
            def _(u=u):
                for fn in fns:
                    fn(u, s)

    @pl.when(c == o[0])
    def _():
        solve(0)

    give_row(0)
    take_row(0)
    send_lower(0, range(U // 2 - 1, -1, -1))
    send_lower(1, range(U - 1, -1, -1))
    send_plain(1)

    q1 = (d[1] - r) // C
    first = c == o[1]

    def picked(u):
        return first & (q1 == u)

    for u in range(U // 2 - 1, U):
        collect(u, 0, picked(u))

        @pl.when(picked(u))
        def _(u=u):
            right(u, 0)
            left(u, 0)

    @pl.when(first)
    def _():
        solve(1)

    give_row(1)

    def rest():
        on_targets(0, (right, left), picked)

    for u in range(U):
        collect(u, 0, jnp.logical_not(picked(u)))
    rest()

    take_row(1)
    on_targets(1, (right,))
    for u in range(U):
        collect(u, 1)
    on_targets(1, (left,))

    for cond, copy in sends:
        @pl.when(cond)
        def _(copy=copy):
            copy.wait_send()


def on_device(state, coupling, coupling_t, factor, cofactor, rates):
    R = lax.axis_size("row")
    C = lax.axis_size("col")
    U = 2 * R // C
    BS = state.shape[0]
    SR = factor.shape[2]
    flat = U * BS
    vmem = pl.BlockSpec(memory_space=pltpu.VMEM)
    n_sends = 2 * STEPS * (2 * U) + (STEPS + 8) * (2 * U) + STEPS * CHUNKS * (R + 2 * U + 8)
    dma = pltpu.SemaphoreType.DMA
    out = pl.pallas_call(
        functools.partial(kernel, R, C, U, BS, SR),
        out_shape=jax.ShapeDtypeStruct((BS, flat), F32),
        in_specs=[vmem] * 6,
        out_specs=vmem,
        scratch_shapes=[
            pltpu.VMEM((4, BS, BS), F32),
            pltpu.VMEM((U, BS), F32),
            pltpu.VMEM((STEPS, U + 1, BS, BS), F32),
            pltpu.VMEM((STEPS, U, BS, BS), jnp.bfloat16),
            pltpu.VMEM((U, BS, BS), jnp.bfloat16),
            dma((4,)),
            dma((1,)),
            dma((STEPS, U + 1, CHUNKS)),
            dma((STEPS, U)),
            dma((U,)),
            dma((n_sends,)),
        ],
        compiler_params=pltpu.CompilerParams(
            collective_id=0, has_side_effects=True, vmem_limit_bytes=48 * 1024 * 1024),
    )(
        state.reshape(BS, flat),
        coupling.reshape(BS, flat),
        coupling_t[0].reshape(BS, flat),
        factor.reshape(U, SR, BS),
        cofactor.reshape(U, SR, BS),
        rates.reshape(U, BS),
    )
    return out.reshape(BS, 1, flat)


def solution(mesh):
    return jax.shard_map(
        on_device,
        mesh=mesh,
        in_specs=(
            P("row", "col", None),
            P("row", "col", None),
            P(None, "row", "col", None),
            P(None, "col", "row", None),
            P(None, "col", "row", None),
            P(None, "col", None),
        ),
        out_specs=P("row", "col", None),
        check_vma=False,
    )
```

```python
import functools

import jax
import jax.numpy as jnp
from jax import lax
from jax.experimental import pallas as pl
from jax.experimental.pallas import tpu as pltpu
from jax.sharding import PartitionSpec as P

STEPS = 2
CHUNKS = 4
MESH = pl.DeviceIdType.MESH
F32 = jnp.float32
NN = (((1,), (0,)), ((), ()))
NT = (((1,), (1,)), ((), ()))


def halves(x):
    hi = x.astype(jnp.bfloat16)
    return hi, (x - hi.astype(F32)).astype(jnp.bfloat16)


def mm(a, b, dims):
    return lax.dot_general(a, b, dims, preferred_element_type=F32)


def dot3(a, b, dims):
    ah, al = halves(a)
    bh, bl = halves(b)
    return mm(ah, bh, dims) + (mm(ah, bl, dims) + mm(al, bh, dims))


def kernel(R, C, U, BS, SR, state, upper, lower, factor, cofactor, rates, out,
           ops, ebuf, xz, atb, an, ops_sem, e_sem, xz_sem, at_sem, an_sem, send_sem):
    H = R // 2
    r = lax.axis_index("row")
    c = lax.axis_index("col")
    d = [2 * R - 1 - s for s in range(STEPS)]

    def owner(row, s):
        return (d[s] - row) % C

    o = [owner(r, s) for s in range(STEPS)]
    sends = []
    me = r * C + c

    barrier = pltpu.get_barrier_semaphore()

    @pl.loop(1, R * C)
    def _(k):
        peer = (me + k) % (R * C)
        pl.semaphore_signal(barrier, inc=1, device_id=(peer // C, peer % C), device_id_type=MESH)

    pl.semaphore_wait(barrier, R * C - 1)

    def send(cond, src, dst, sem, dev):
        k = len(sends)
        copy = pltpu.make_async_remote_copy(
            src_ref=src, dst_ref=dst, send_sem=send_sem.at[k], recv_sem=sem,
            device_id=dev, device_id_type=MESH)
        sends.append((cond, copy))

        @pl.when(cond)
        def _():
            copy.start()

    def send_or_local(cond, src, dst, sem, dev):
        mine = (dev[0] == r) & (dev[1] == c)
        send(cond & jnp.logical_not(mine), src, dst, sem, dev)

        @pl.when(cond & mine)
        def _():
            pltpu.make_async_copy(src, dst, sem).start()

    def arrive(ref, sem):
        pltpu.make_async_copy(ref, ref, sem).wait()

    def slot(u):
        if isinstance(u, int):
            return pl.ds(u * BS, BS)
        return pl.ds(pl.multiple_of(u * BS, BS), BS)

    def target(row, m, s):
        return (row <= m) & (row + m < d[s])

    rows = pl.ds(pl.multiple_of(r * SR, SR), SR)

    def send_operators(s):
        for src, base in ((cofactor, 0), (factor, 2)):
            for u in range(U):
                m = c + C * u
                if u >= U // 2 - s:
                    to = d[s] - m
                    send_or_local((to >= 0) & (to < R), src.at[u], ops.at[base + 1, rows],
                                  ops_sem.at[base + 1], (to, c))
                if u < U // 2:
                    send_or_local(m < R, src.at[u], ops.at[base, rows],
                                  ops_sem.at[base], (m, owner(m, s)))

    def from_upper(u):
        return (u + 1) * C <= H

    def send_lower(s, slots):
        to = (r + R - s - H) % R
        for u in slots:
            if not from_upper(u):
                m = c + C * u
                send(target(to, m, s) & (to + s < R), lower.at[0, :, slot(u)], atb.at[s, u],
                     at_sem.at[s, u], (to, c))

    def send_plain(s):
        m = r
        to_u = jnp.minimum(m // C, U - 1)
        for u in range(H // C + 1):
            i = c + C * u - s
            reach = (i >= 0) & (m < (H // C) * C) & target(i, m, s)
            send_or_local(reach, upper.at[:, slot(u)], atb.at[s, to_u],
                          at_sem.at[s, to_u], (i, m % C))

    def send_upper():
        for u in range(U):
            m = c + C * u - 1
            to = (c + C - 1) % C
            to_u = jnp.maximum(jnp.where(c >= 1, u, u - 1), 0)
            send((m >= 0) & target(r, m, 1), upper.at[:, slot(u)], an.at[to_u],
                 an_sem.at[to_u], (r, to))

    for s in range(STEPS):
        send_or_local(c == r % C, rates, ebuf, e_sem.at[0], (r, o[s]))
    send_operators(0)
    send_operators(1)
    send_upper()
    send_lower(0, range(U - 1, U // 2 - 1, -1))
    send_plain(0)
    out[...] = state[...]

    def spread(s, h, who):
        own_col = r % C == c
        k = jnp.where(own_col, r // C, (d[s] - r) // C)
        has = (own_col | (c == o[s])) & who

        def give(cond, to):
            send(cond & has, xz.at[s, U, part(h)], xz.at[s, k, part(h)], xz_sem.at[s, k, h], (to, c))

        give(r % 2 == 1, jnp.maximum(r - 1, 0))
        for back in range(1, R // 2):
            pair = r // 2 - back
            give(pair >= 0, jnp.maximum(2 * pair + 1 - r % 2, 0))

    def part(h):
        return pl.ds(h * (BS // CHUNKS), BS // CHUNKS)

    def pass_row(s, h, who=True):
        block = xz.at[s, U, part(h)]
        sem = xz_sem.at[s, U, h]
        far = o[s] == 0
        up = (c >= o[s]) & (c < C - 1)
        if s == 0:
            send((c == o[s]) & far & who, block, block, sem, (r, C - 1))
            up = up & jnp.logical_not(far & (c == C - 2))
        send((c <= o[s]) & (c >= 1) & who, block, block, sem, (r, jnp.maximum(c - 1, 0)))
        send(up & who, block, block, sem, (r, jnp.minimum(c + 1, C - 1)))

    def take_row(s):
        other = c != o[s]
        for h in range(CHUNKS):
            @pl.when(other)
            def _(h=h):
                arrive(xz.at[s, U, part(h)], xz_sem.at[s, U, h])

            pass_row(s, h, other)
            spread(s, h, other)

    def give_row(s):
        for h in range(CHUNKS):
            pass_row(s, h, c == o[s])
            spread(s, h, c == o[s])

    def solve(s):
        q = (d[s] - r) // C
        arrive(ebuf, e_sem.at[0])
        left_e = jnp.transpose(jnp.broadcast_to(ebuf[pl.ds(r // C, 1), :], (BS, BS)))
        rate = left_e + rates[pl.ds(q, 1), :]
        arrive(ops.at[0], ops_sem.at[0])
        mid = dot3(ops[0], out[:, slot(q)], NN)
        arrive(ops.at[1], ops_sem.at[1])
        mid = dot3(mid, ops[1], NT) / rate
        arrive(ops.at[2], ops_sem.at[2])
        mid = dot3(ops[2], mid, NN)
        arrive(ops.at[3], ops_sem.at[3])
        x = -dot3(mid, ops[3], NT)
        xz[s, U] = x
        out[:, slot(q)] = x

    def z_index(u, s):
        m = c + C * u
        j = jnp.where(d[s] - m <= m, d[s] - m, m)
        k = jnp.where(j == r, U, jnp.where(j % C == c, j // C, u))
        return j, k

    def collect(u, s, extra=True):
        j, k = z_index(u, s)
        landed = r < j
        if u >= U // 2:
            landed = landed & (j % C != c)
        landed = landed & extra

        for h in range(CHUNKS):
            block = xz.at[s, u, part(h)]

            @pl.when(landed)
            def _(block=block, h=h):
                arrive(block, xz_sem.at[s, u, h])

            send(landed & (r // 2 < j // 2) & (r % 2 != j % 2), block, block,
                 xz_sem.at[s, u, h], (r + 1 - 2 * (r % 2), c))

    def right(u, s):
        arrive(atb.at[s, u], at_sem.at[s, u])
        xh, xl = halves(xz[s, U])
        at = atb[s, u]
        dims = NT if from_upper(u) else NN
        out[:, slot(u)] -= mm(xh, at, dims) + mm(xl, at, dims)

    def left(u, s):
        m = c + C * u
        j, k = z_index(u, s)
        if s > 0:
            arrive(an.at[u], an_sem.at[u])
            a = an[u]
        else:
            a = upper[:, slot(u)]
        zh, zl = halves(xz[s, k])

        def apply(dims):
            out[:, slot(u)] -= mm(a, zh, dims) + mm(a, zl, dims)

        low, high = C * u, C * u + C - 1
        if 2 * low >= d[s]:
            apply(NN)
        elif 2 * high < d[s]:
            apply(NT)
        else:
            straight = d[s] - m <= m
            pl.when(straight)(lambda: apply(NN))
            pl.when(jnp.logical_not(straight))(lambda: apply(NT))

    def on_targets(s, fns, but=None):
        for u in range(U):
            live = target(r, c + C * u, s)
            if but is not None:
                live = live & jnp.logical_not(but(u))

            @pl.when(live)
            def _(u=u):
                for fn in fns:
                    fn(u, s)

    @pl.when(c == o[0])
    def _():
        solve(0)

    give_row(0)
    take_row(0)
    send_lower(0, range(U // 2 - 1, -1, -1))
    send_lower(1, range(U - 1, -1, -1))
    send_plain(1)

    q1 = (d[1] - r) // C
    first = c == o[1]

    def picked(u):
        return first & (q1 == u)

    for u in range(U // 2 - 1, U):
        collect(u, 0, picked(u))

        @pl.when(picked(u))
        def _(u=u):
            right(u, 0)
            left(u, 0)

    @pl.when(first)
    def _():
        solve(1)

    give_row(1)

    def rest():
        on_targets(0, (right, left), picked)

    for u in range(U):
        collect(u, 0, jnp.logical_not(picked(u)))
    rest()

    take_row(1)
    on_targets(1, (right,))
    for u in range(U):
        collect(u, 1)
    on_targets(1, (left,))

    for cond, copy in sends:
        @pl.when(cond)
        def _(copy=copy):
            copy.wait_send()


def on_device(state, coupling, coupling_t, factor, cofactor, rates):
    R = lax.axis_size("row")
    C = lax.axis_size("col")
    U = 2 * R // C
    BS = state.shape[0]
    SR = factor.shape[2]
    flat = U * BS
    vmem = pl.BlockSpec(memory_space=pltpu.VMEM)
    hbm = pl.BlockSpec(memory_space=pl.ANY)
    n_sends = 2 * STEPS * (2 * U) + (STEPS + 8) * (2 * U) + STEPS * CHUNKS * (R + 2 * U + 8)
    dma = pltpu.SemaphoreType.DMA
    out = pl.pallas_call(
        functools.partial(kernel, R, C, U, BS, SR),
        out_shape=jax.ShapeDtypeStruct((BS, flat), F32),
        in_specs=[vmem, vmem, hbm, vmem, vmem, vmem],
        out_specs=vmem,
        scratch_shapes=[
            pltpu.VMEM((4, BS, BS), F32),
            pltpu.VMEM((U, BS), F32),
            pltpu.VMEM((STEPS, U + 1, BS, BS), F32),
            pltpu.VMEM((STEPS, U, BS, BS), jnp.bfloat16),
            pltpu.VMEM((U, BS, BS), jnp.bfloat16),
            dma((4,)),
            dma((1,)),
            dma((STEPS, U + 1, CHUNKS)),
            dma((STEPS, U)),
            dma((U,)),
            dma((n_sends,)),
        ],
        compiler_params=pltpu.CompilerParams(
            collective_id=0, has_side_effects=True, vmem_limit_bytes=48 * 1024 * 1024),
    )(
        state.reshape(BS, flat),
        coupling.reshape(BS, flat),
        coupling_t.reshape(coupling_t.shape[0], BS, flat),
        factor.reshape(U, SR, BS),
        cofactor.reshape(U, SR, BS),
        rates.reshape(U, BS),
    )
    return out.reshape(BS, 1, flat)


def solution(mesh):
    return jax.shard_map(
        on_device,
        mesh=mesh,
        in_specs=(
            P("row", "col", None),
            P("row", "col", None),
            P(None, "row", "col", None),
            P(None, "col", "row", None),
            P(None, "col", "row", None),
            P(None, "col", None),
        ),
        out_specs=P("row", "col", None),
        check_vma=False,
    )
```
